8 devices in a mesh: dp: 1 (over z), sp: 2 (over y), tp: 4 (over x, core).
Axes of the slice: x: 2, y: 2, z: 1, core: 2. Of those that a mesh axis runs over, the one named last changes fastest.
Arguments:
- x_seq: bfloat16 [2, 512, 8192], P('dp', ('sp', 'tp'))
- w_zx: bfloat16 [8192, 2, 16384], P(None, None, 'tp')
- w_dt: bfloat16 [8192, 256], P(None, 'tp')
- w_bc: bfloat16 [8192, 2, 8, 256], replicated
- conv_x: bfloat16 [4, 16384], P(None, 'tp')
- conv_bc: bfloat16 [4, 2, 8, 256], replicated
- bias_x: bfloat16 [16384], P('tp')
- bias_bc: bfloat16 [2, 8, 256], replicated
- a_log: float32 [256], P('tp')
- dt_bias: float32 [256], P('tp')
- d_skip: float32 [256], P('tp')
- norm_w: bfloat16 [16384], P('tp')
- w_out: bfloat16 [16384, 8192], P('tp')
Outputs:
- output: bfloat16 [2, 512, 8192], P('dp', ('sp', 'tp'))
All inputs are finite; a program needn't handle non-finite values.
Results may differ from the reference program's by a relative error of at most 0.00554757.
Values are sent between devices in bfloat16 or wider.
A program may use at most 1.25 GiB of HBM per device.

```python
import math
import jax
import jax.numpy as jnp
from jax import lax

DMODEL = 8192
HEADS = 256
GROUPS = 8
HEAD = 64
STATE = 256
BLOCK = 256
SEQ = 512
TILE = 256
SEQS = 2


def setup_inputs(seed: int = 0, part: int = 0) -> dict:
    inner_dim = HEADS * HEAD
    sub_keys = jax.random.split(jax.random.key(seed), 14)
    part_key = jax.random.fold_in(jax.random.key(seed + 1), part)
    scale_in = DMODEL ** -0.5
    x_seq = jax.random.normal(part_key, (SEQS, SEQ, DMODEL), jnp.float32)
    head_gain = jnp.exp(jax.random.uniform(sub_keys[0], (HEADS, 1), jnp.float32, -0.7, 0.7))
    z_gain = jnp.broadcast_to(head_gain, (HEADS, HEAD)).reshape(1, 1, inner_dim)
    w_zx = jax.random.normal(sub_keys[1], (DMODEL, 2, inner_dim), jnp.float32) * scale_in
    w_zx = w_zx * jnp.concatenate([z_gain, jnp.ones_like(z_gain)], axis=1)
    w_dt = jax.random.normal(sub_keys[2], (DMODEL, HEADS), jnp.float32) * (0.5 * scale_in)
    w_bc = jax.random.normal(sub_keys[3], (DMODEL, 2, GROUPS, STATE), jnp.float32) * scale_in
    conv_x = jax.random.normal(sub_keys[4], (4, inner_dim), jnp.float32) * 0.5
    conv_bc = jax.random.normal(sub_keys[5], (4, 2, GROUPS, STATE), jnp.float32) * 0.5
    bias_x = jax.random.normal(sub_keys[6], (inner_dim,), jnp.float32) * 0.7
    bias_bc = jax.random.normal(sub_keys[7], (2, GROUPS, STATE), jnp.float32) * 0.7
    a_log = math.log(0.5) + jax.random.uniform(sub_keys[8], (HEADS,), jnp.float32, -0.7, 0.7)
    dt_bias = jax.random.uniform(sub_keys[9], (HEADS,), jnp.float32, -0.5, 0.5) - math.log(BLOCK)
    d_skip = 2.5 + jax.random.normal(sub_keys[10], (HEADS,), jnp.float32)
    norm_w = jax.random.uniform(sub_keys[11], (inner_dim,), jnp.float32, 0.5, 1.5)
    w_out = jax.random.normal(sub_keys[12], (inner_dim, DMODEL), jnp.float32) * inner_dim ** -0.5
    return dict(x_seq=x_seq.astype(jnp.bfloat16), w_zx=w_zx.astype(jnp.bfloat16), w_dt=w_dt.astype(jnp.bfloat16), w_bc=w_bc.astype(jnp.bfloat16), conv_x=conv_x.astype(jnp.bfloat16), conv_bc=conv_bc.astype(jnp.bfloat16), bias_x=bias_x.astype(jnp.bfloat16), bias_bc=bias_bc.astype(jnp.bfloat16), a_log=a_log, dt_bias=dt_bias, d_skip=d_skip, norm_w=norm_w.astype(jnp.bfloat16), w_out=w_out.astype(jnp.bfloat16))


def reference(x_seq, w_zx, w_dt, w_bc, conv_x, conv_bc, bias_x, bias_bc, a_log, dt_bias, d_skip, norm_w, w_out):
    inner_dim = HEADS * HEAD
    half_bc = GROUPS * STATE
    chan_dim = inner_dim + 2 * half_bc
    per_group = HEADS // GROUPS
    n_tiles = SEQ // TILE
    w_proj = jnp.concatenate([w_zx.reshape(DMODEL, 2 * inner_dim), w_bc.reshape(DMODEL, 2 * half_bc), w_dt], axis=1)
    conv_w = jnp.concatenate([conv_x, conv_bc.reshape(4, 2 * half_bc)], axis=1).astype(jnp.float32)
    conv_b = jnp.concatenate([bias_x, bias_bc.reshape(2 * half_bc)]).astype(jnp.float32)
    a_rate = jnp.exp(a_log)
    causal = (jnp.arange(TILE)[:, None] >= jnp.arange(TILE)[None, :])[None, :, :, None]
    x_tiles = x_seq.reshape(SEQS, n_tiles, TILE, DMODEL).transpose(1, 0, 2, 3)

    def tile_step(carry_in, x_tile):
        conv_tail, ssm_state = carry_in
        proj_out = jnp.dot(x_tile.reshape(SEQS * TILE, DMODEL), w_proj, preferred_element_type=jnp.float32)
        proj_out = proj_out.astype(jnp.bfloat16).reshape(SEQS, TILE, inner_dim + chan_dim + HEADS)
        gate_z = proj_out[:, :, :inner_dim].astype(jnp.float32)
        pre_conv = proj_out[:, :, inner_dim:inner_dim + chan_dim]
        dt_raw = proj_out[:, :, inner_dim + chan_dim:].astype(jnp.float32)
        padded = jnp.concatenate([conv_tail, pre_conv], axis=1).astype(jnp.float32)
        conv_sum = conv_b + sum(padded[:, tap_idx:tap_idx + TILE] * conv_w[tap_idx] for tap_idx in range(4))
        act_vals = jax.nn.silu(conv_sum).astype(jnp.bfloat16).astype(jnp.float32)
        x_in = act_vals[:, :, :inner_dim].reshape(SEQS, TILE, HEADS, HEAD)
        b_heads = jnp.repeat(act_vals[:, :, inner_dim:inner_dim + half_bc].reshape(SEQS, TILE, GROUPS, STATE), per_group, axis=2)
        c_heads = jnp.repeat(act_vals[:, :, inner_dim + half_bc:].reshape(SEQS, TILE, GROUPS, STATE), per_group, axis=2)
        dt_vals = jax.nn.softplus(dt_raw + dt_bias)
        cum_log = jnp.cumsum(-a_rate * dt_vals, axis=1)
        log_diff = cum_log[:, :, None, :] - cum_log[:, None, :, :]
        decay_mat = jnp.where(causal, jnp.exp(jnp.where(causal, log_diff, 0.0)), 0.0)
        scores = jnp.einsum('athn,ashn->atsh', c_heads, b_heads)
        weights = scores * decay_mat * dt_vals[:, None, :, :]
        y_diag = jnp.einsum('atsh,ashp->athp', weights, x_in)
        y_prev = jnp.einsum('athn,ahpn->athp', c_heads, ssm_state) * jnp.exp(cum_log)[..., None]
        y_all = y_diag + y_prev + d_skip[:, None] * x_in
        tile_end = cum_log[:, -1, :]
        weighted_x = x_in * (jnp.exp(tile_end[:, None, :] - cum_log) * dt_vals)[..., None]
        new_state = jnp.exp(tile_end)[:, :, None, None] * ssm_state + jnp.einsum('ashp,ashn->ahpn', weighted_x, b_heads)
        gated_y = y_all.reshape(SEQS, TILE, inner_dim) * jax.nn.silu(gate_z)
        grouped = gated_y.reshape(SEQS, TILE, GROUPS, inner_dim // GROUPS)
        inv_rms = lax.rsqrt(jnp.mean(jnp.square(grouped), axis=-1, keepdims=True) + 1e-5)
        normed = ((grouped * inv_rms).reshape(SEQS, TILE, inner_dim) * norm_w.astype(jnp.float32)).astype(jnp.bfloat16)
        out_tile = jnp.dot(normed.reshape(SEQS * TILE, inner_dim), w_out, preferred_element_type=jnp.float32)
        y_tile = (x_tile.astype(jnp.float32) + out_tile.reshape(SEQS, TILE, DMODEL)).astype(jnp.bfloat16)
        return (padded[:, TILE:].astype(jnp.bfloat16), new_state), y_tile

    init_carry = (jnp.zeros((SEQS, 3, chan_dim), jnp.bfloat16), jnp.zeros((SEQS, HEADS, HEAD, STATE), jnp.float32))
    y_tiles = lax.scan(tile_step, init_carry, x_tiles)[1]
    return y_tiles.transpose(1, 0, 2, 3).reshape(SEQS, SEQ, DMODEL)
```

```python
import functools

import jax
import jax.numpy as jnp
from jax import lax
from jax.experimental import pallas as pl
from jax.experimental.pallas import tpu as pltpu
from jax.sharding import PartitionSpec as P

MESH = pl.DeviceIdType.MESH
CHUNK = 128
NB = 512
F32 = jnp.float32
BF16 = jnp.bfloat16


def silu(v):
    return v * jax.nn.sigmoid(v)


def ssd_kernel(z_ref, x_ref, bc_ref, r_ref, prm_ref, bcp_ref, hp_ref, q_ref, xs, bs, state, qs, prev):
    chunk = pl.program_id(1)
    T = CHUNK
    width = xs.shape[1]

    @pl.when(chunk == 0)
    def _():
        xs[0:8, :] = jnp.zeros((8, width), F32)
        bs[0:8, :] = jnp.zeros((8, bs.shape[1]), F32)
        state[...] = jnp.zeros_like(state)

    @pl.when(chunk > 0)
    def _():
        xs[0:8, :] = xs[T:T + 8, :]
        bs[0:8, :] = bs[T:T + 8, :]

    xs[8:8 + T, :] = x_ref[0].astype(F32)
    bs[8:8 + T, :] = bc_ref[0].astype(F32)

    conv_bc = bcp_ref[0, 4:5, :]
    for tap in range(4):
        conv_bc = conv_bc + bs[5 + tap:5 + tap + T, :] * bcp_ref[0, tap:tap + 1, :]
    bc_act = silu(conv_bc).astype(BF16)
    n_state = bc_act.shape[1] // 2
    b_mat, c_mat = bc_act[:, :n_state], bc_act[:, n_state:]
    scores = lax.dot_general(c_mat, b_mat, (((1,), (1,)), ((), ())), preferred_element_type=F32)
    b_t = jnp.transpose(b_mat.astype(F32)).astype(BF16)

    dt = jax.nn.softplus(r_ref[0].astype(F32) + hp_ref[0, 0:1, :])
    log_a = hp_ref[0, 1:2, :] * dt
    row = lax.broadcasted_iota(jnp.int32, (T, T), 0)
    col = lax.broadcasted_iota(jnp.int32, (T, T), 1)
    causal = row >= col
    cum = jnp.dot(causal.astype(F32), log_a, preferred_element_type=F32, precision=lax.Precision.HIGHEST)
    cum_t = jnp.transpose(cum)
    dt_t = jnp.transpose(dt)
    left = lax.broadcasted_iota(jnp.int32, (T, 128), 1) < 64
    prev[...] = jnp.dot(c_mat, state[...].astype(BF16), preferred_element_type=F32)
    sq = jnp.zeros((T, 128), F32)

    for pair in range(width // 128):
        lanes = slice(pair * 128, pair * 128 + 128)
        conv = prm_ref[4:5, lanes]
        for tap in range(4):
            conv = conv + xs[5 + tap:5 + tap + T, lanes] * prm_ref[tap:tap + 1, lanes]
        u = silu(conv).astype(BF16)
        u32 = u.astype(F32)
        parts, cums, dts = [], [], []
        for half in range(2):
            h = 2 * pair + half
            cum_b = jnp.broadcast_to(cum[:, h:h + 1], (T, 128))
            decay = jnp.exp(jnp.where(causal, cum_b - cum_t[h:h + 1, :], -1e30))
            w = scores * decay * dt_t[h:h + 1, :]
            parts.append(jnp.dot(w.astype(BF16), u, preferred_element_type=F32))
            cums.append(cum_b)
            dts.append(jnp.broadcast_to(dt[:, h:h + 1], (T, 128)))
        cum_p = jnp.where(left, cums[0], cums[1])
        dt_p = jnp.where(left, dts[0], dts[1])
        end = cum_p[T - 1:T, :]
        y = jnp.where(left, parts[0], parts[1]) + jnp.exp(cum_p) * prev[:, lanes] + prm_ref[6:7, lanes] * u32
        xw = (u32 * (jnp.exp(end - cum_p) * dt_p)).astype(BF16)
        state[:, lanes] = jnp.exp(end) * state[:, lanes] + jnp.dot(b_t, xw, preferred_element_type=F32)
        gated = y * silu(z_ref[0, :, lanes].astype(F32))
        qs[:, lanes] = gated
        sq = sq + gated * gated

    inv = lax.rsqrt(jnp.sum(sq, axis=1, keepdims=True) / width + 1e-5)
    q_ref[...] = (qs[...] * inv * prm_ref[5:6, :]).astype(BF16)


def ssd_call(zx, bc, r, prm, bcp, hp):
    n_tok, inner = zx.shape[1], zx.shape[2]
    groups = bc.shape[0]
    width = inner // groups
    n_bc = bc.shape[2]
    T = CHUNK
    return pl.pallas_call(
        ssd_kernel,
        grid=(groups, n_tok // T),
        in_specs=[
            pl.BlockSpec((1, T, width), lambda g, c: (0, c, g)),
            pl.BlockSpec((1, T, width), lambda g, c: (1, c, g)),
            pl.BlockSpec((1, T, n_bc), lambda g, c: (g, c, 0)),
            pl.BlockSpec((1, T, 128), lambda g, c: (g, c, 0)),
            pl.BlockSpec((8, width), lambda g, c: (0, g)),
            pl.BlockSpec((1, 8, n_bc), lambda g, c: (g, 0, 0)),
            pl.BlockSpec((1, 8, 128), lambda g, c: (g, 0, 0)),
        ],
        out_specs=pl.BlockSpec((T, width), lambda g, c: (c, g)),
        out_shape=jax.ShapeDtypeStruct((n_tok, inner), BF16),
        scratch_shapes=[
            pltpu.VMEM((T + 8, width), F32),
            pltpu.VMEM((T + 8, n_bc), F32),
            pltpu.VMEM((n_bc // 2, width), F32),
            pltpu.VMEM((T, width), F32),
            pltpu.VMEM((T, width), F32),
        ],
        compiler_params=pltpu.CompilerParams(dimension_semantics=('arbitrary', 'arbitrary'), vmem_limit_bytes=48 * 2**20),
        cost_estimate=pl.CostEstimate(flops=8 * 10**9, bytes_accessed=14 * 2**20, transcendentals=10**7),
        name='ssd',
    )(zx, zx, bc, r, prm, bcp, hp)


def out_kernel(n_blk, rows, q_hbm, res_ref, w_ref, out_ref, qp, snd, own, rxs, rxx, ysnd, yrx, qsem, ss, rs, xs, xr, ys, yr):
    p, n = pl.program_id(0), pl.program_id(1)
    dp, sp, tp = lax.axis_index('dp'), lax.axis_index('sp'), lax.axis_index('tp')
    core = lax.rem(tp, 2)
    sib = tp + 1 - 2 * core
    across = lax.rem(tp + 2, 4)
    diag = lax.rem(sib + 2, 4)
    to_sib, to_x, to_y = (dp, sp, sib), (dp, sp, across), (dp, 1 - sp, tp)

    def q_copies(which):
        out = []
        for slot, quarter in enumerate(((diag, across), (sib, tp))[which]):
            for blk in range(2):
                src = q_hbm.at[pl.ds(pl.multiple_of(blk * 4 * rows + quarter * rows, rows), rows)]
                dst = qp.at[which, pl.ds((slot * 2 + blk) * rows, rows)]
                out.append(pltpu.make_async_copy(src, dst, qsem.at[which * 4 + slot * 2 + blk]))
        return out

    def sib_copy(k, m):
        return pltpu.make_async_remote_copy(
            src_ref=snd.at[k, m], dst_ref=rxs.at[k, m], send_sem=ss.at[k, m], recv_sem=rs.at[k, m],
            device_id=to_sib, device_id_type=MESH)

    def x_copy(m):
        return pltpu.make_async_remote_copy(
            src_ref=own.at[0, m], dst_ref=rxx.at[m], send_sem=xs.at[m], recv_sem=xr.at[m],
            device_id=to_x, device_id_type=MESH)

    def y_copy(m):
        return pltpu.make_async_remote_copy(
            src_ref=ysnd.at[m], dst_ref=yrx.at[m], send_sem=ys.at[m], recv_sem=yr.at[m],
            device_id=to_y, device_id_type=MESH)

    @pl.when(jnp.logical_and(p == 0, n == 0))
    def _():
        for copy in q_copies(0) + q_copies(1):
            copy.start()
        barrier = pltpu.get_barrier_semaphore()
        for peer in (to_sib, to_x, to_y):
            pl.semaphore_signal(barrier, inc=1, device_id=peer, device_id_type=MESH)
        pl.semaphore_wait(barrier, 3)
        for copy in q_copies(0) + q_copies(1):
            copy.wait()

    acc = jnp.dot(qp[p], w_ref[...], preferred_element_type=F32)
    snd[p, n] = acc[:2 * rows]
    own[p, n] = acc[2 * rows:]
    sib_copy(p, n).start()

    def forward(m):
        sib_copy(0, m).wait_recv()
        own[0, m] = own[0, m] + rxs[0, m]
        x_copy(m).start()

    @pl.when(jnp.logical_and(p == 0, n >= 1))
    def _():
        forward(n - 1)

    @pl.when(jnp.logical_and(p == 1, n == 0))
    def _():
        forward(n_blk - 1)

    @pl.when(jnp.logical_and(p == 1, n == n_blk - 1))
    def _():
        def finish(m, carry):
            sib_copy(1, m).wait_recv()
            x_copy(m).wait_recv()
            cols = pl.ds(pl.multiple_of(m * NB, NB), NB)
            for half, blk in enumerate((sp, 1 - sp)):
                part = pl.ds(pl.multiple_of(blk * rows, rows), rows)
                total = own[1, m, part] + rxs[1, m, part] + rxx[m, part] + res_ref[part, cols].astype(F32)
                if half == 0:
                    out_ref[sp, :, cols] = total.astype(BF16)
                else:
                    ysnd[m] = total.astype(BF16)
            y_copy(m).start()
            return carry

        lax.fori_loop(0, n_blk, finish, 0)

        def drain(m, carry):
            y_copy(m).wait_recv()
            cols = pl.ds(pl.multiple_of(m * NB, NB), NB)
            out_ref[1 - sp, :, cols] = yrx[m]
            sib_copy(0, m).wait_send()
            sib_copy(1, m).wait_send()
            x_copy(m).wait_send()
            y_copy(m).wait_send()
            return carry

        lax.fori_loop(0, n_blk, drain, 0)


def out_call(q, res, w_out):
    depth, d_model = w_out.shape
    rows = res.shape[0] // 2
    n_blk = d_model // NB
    blk2 = (2, n_blk, 2 * rows, NB)
    return pl.pallas_call(
        functools.partial(out_kernel, n_blk, rows),
        grid=(2, n_blk),
        in_specs=[
            pl.BlockSpec(memory_space=pl.ANY),
            pl.BlockSpec(memory_space=pltpu.VMEM),
            pl.BlockSpec((depth, NB), lambda p, n: (0, n)),
        ],
        out_specs=pl.BlockSpec(memory_space=pltpu.VMEM),
        out_shape=jax.ShapeDtypeStruct((2, rows, d_model), BF16),
        scratch_shapes=[
            pltpu.VMEM((2, 4 * rows, depth), BF16),
            pltpu.VMEM(blk2, F32),
            pltpu.VMEM(blk2, F32),
            pltpu.VMEM(blk2, F32),
            pltpu.VMEM(blk2[1:], F32),
            pltpu.VMEM((n_blk, rows, NB), BF16),
            pltpu.VMEM((n_blk, rows, NB), BF16),
            pltpu.SemaphoreType.DMA((8,)),
            pltpu.SemaphoreType.DMA((2, n_blk)),
            pltpu.SemaphoreType.DMA((2, n_blk)),
            pltpu.SemaphoreType.DMA((n_blk,)),
            pltpu.SemaphoreType.DMA((n_blk,)),
            pltpu.SemaphoreType.DMA((n_blk,)),
            pltpu.SemaphoreType.DMA((n_blk,)),
        ],
        compiler_params=pltpu.CompilerParams(
            dimension_semantics=('arbitrary', 'arbitrary'), collective_id=1, has_side_effects=True, vmem_limit_bytes=60 * 2**20),
        cost_estimate=pl.CostEstimate(flops=35 * 10**9, bytes_accessed=140 * 2**20, transcendentals=0),
        name='out_proj',
    )(q, res, w_out)


def solution(mesh):
    tp_size = mesh.shape['tp']
    tok_spec = P('dp', ('sp', 'tp'), None)

    def local_layer(x_loc, w_zx, w_dt, w_bc, conv_x, conv_bc, bias_x, bias_bc, a_log, dt_bias, d_skip, norm_w, w_out):
        rows, d_model = x_loc.shape[1], x_loc.shape[2]
        groups = w_bc.shape[2]
        heads = a_log.shape[0]
        inner = w_zx.shape[2]
        g_loc = groups // tp_size
        per_group = heads // g_loc
        sp, tp = lax.axis_index('sp'), lax.axis_index('tp')
        first = tp * g_loc
        w_bc_loc = lax.dynamic_slice_in_dim(w_bc, first, g_loc, axis=2)
        conv_bc_loc = lax.dynamic_slice_in_dim(conv_bc, first, g_loc, axis=2)
        bias_bc_loc = lax.dynamic_slice_in_dim(bias_bc, first, g_loc, axis=1)

        mine = jnp.where(sp == 0, x_loc[0], x_loc[1])
        other = jnp.where(sp == 0, x_loc[1], x_loc[0])
        got = lax.ppermute(other, 'sp', [(0, 1), (1, 0)])
        x_pair = jnp.stack([jnp.where(sp == 0, mine, got), jnp.where(sp == 0, got, mine)])
        x_all = lax.all_gather(x_pair, 'tp', axis=1, tiled=True).reshape(-1, d_model)

        n_tok = x_all.shape[0]
        n_state = w_bc.shape[3]
        bc = jnp.einsum('md,dcgn->gmcn', x_all, w_bc_loc, preferred_element_type=F32).astype(BF16)
        bc = bc.reshape(g_loc, n_tok, 2 * n_state)
        r = jnp.einsum('md,dh->mh', x_all, w_dt, preferred_element_type=F32).astype(BF16)
        r = jnp.moveaxis(r.reshape(n_tok, g_loc, per_group), 1, 0)
        r = jnp.pad(r, ((0, 0), (0, 0), (0, 128 - per_group)))
        zx = jnp.einsum('md,dcn->cmn', x_all, w_zx, preferred_element_type=F32).astype(BF16)

        skip = jnp.repeat(d_skip, inner // heads)
        prm = jnp.concatenate([conv_x.astype(F32), bias_x.astype(F32)[None], norm_w.astype(F32)[None], skip[None], jnp.zeros((1, inner), F32)])
        taps = jnp.moveaxis(conv_bc_loc.astype(F32), 2, 0).reshape(g_loc, 4, 2 * n_state)
        bias = jnp.moveaxis(bias_bc_loc.astype(F32), 1, 0).reshape(g_loc, 1, 2 * n_state)
        bcp = jnp.concatenate([taps, bias, jnp.zeros((g_loc, 3, 2 * n_state), F32)], axis=1)
        hp = jnp.stack([dt_bias, -jnp.exp(a_log)]).reshape(2, g_loc, per_group)
        hp = jnp.pad(jnp.moveaxis(hp, 1, 0), ((0, 0), (0, 6), (0, 128 - per_group)))

        q = ssd_call(zx, bc, r, prm, bcp, hp)
        return out_call(q, x_pair.reshape(2 * rows, d_model), w_out)

    in_specs = (tok_spec, P(None, None, 'tp'), P(None, 'tp'), P(), P(None, 'tp'), P(), P('tp'), P(), P('tp'), P('tp'), P('tp'), P('tp'), P('tp', None))
    return jax.shard_map(local_layer, mesh=mesh, in_specs=in_specs, out_specs=tok_spec, check_vma=False)
```

```python
import functools

import jax
import jax.numpy as jnp
from jax import lax
from jax.experimental import pallas as pl
from jax.experimental.pallas import tpu as pltpu
from jax.sharding import PartitionSpec as P

MESH = pl.DeviceIdType.MESH
CHUNK = 128
NB = 512
F32 = jnp.float32
BF16 = jnp.bfloat16


def silu(v):
    return v * jax.nn.sigmoid(v)


def ssd_kernel(z_ref, x_ref, bc_ref, r_ref, prm_ref, bcp_ref, hp_ref, q_ref, xs, bs, state, qs, prev):
    chunk = pl.program_id(1)
    T = CHUNK
    width = xs.shape[1]

    @pl.when(chunk == 0)
    def _():
        xs[0:8, :] = jnp.zeros((8, width), F32)
        bs[0:8, :] = jnp.zeros((8, bs.shape[1]), F32)
        state[...] = jnp.zeros_like(state)

    @pl.when(chunk > 0)
    def _():
        xs[0:8, :] = xs[T:T + 8, :]
        bs[0:8, :] = bs[T:T + 8, :]

    xs[8:8 + T, :] = x_ref[0].astype(F32)
    bs[8:8 + T, :] = bc_ref[0].astype(F32)

    conv_bc = bcp_ref[0, 4:5, :]
    for tap in range(4):
        conv_bc = conv_bc + bs[5 + tap:5 + tap + T, :] * bcp_ref[0, tap:tap + 1, :]
    bc_act = silu(conv_bc).astype(BF16)
    n_state = bc_act.shape[1] // 2
    b_mat, c_mat = bc_act[:, :n_state], bc_act[:, n_state:]
    scores = lax.dot_general(c_mat, b_mat, (((1,), (1,)), ((), ())), preferred_element_type=F32)
    b_t = jnp.transpose(b_mat.astype(F32)).astype(BF16)

    dt = jax.nn.softplus(r_ref[0].astype(F32) + hp_ref[0, 0:1, :])
    log_a = hp_ref[0, 1:2, :] * dt
    row = lax.broadcasted_iota(jnp.int32, (T, T), 0)
    col = lax.broadcasted_iota(jnp.int32, (T, T), 1)
    causal = row >= col
    cum = jnp.dot(causal.astype(F32), log_a, preferred_element_type=F32, precision=lax.Precision.HIGHEST)
    cum_t = jnp.transpose(cum)
    dt_t = jnp.transpose(dt)
    left = lax.broadcasted_iota(jnp.int32, (T, 128), 1) < 64
    prev[...] = jnp.dot(c_mat, state[...].astype(BF16), preferred_element_type=F32)
    sq = jnp.zeros((T, 128), F32)

    for pair in range(width // 128):
        lanes = slice(pair * 128, pair * 128 + 128)
        conv = prm_ref[4:5, lanes]
        for tap in range(4):
            conv = conv + xs[5 + tap:5 + tap + T, lanes] * prm_ref[tap:tap + 1, lanes]
        u = silu(conv).astype(BF16)
        u32 = u.astype(F32)
        parts, cums, dts = [], [], []
        for half in range(2):
            h = 2 * pair + half
            cum_b = jnp.broadcast_to(cum[:, h:h + 1], (T, 128))
            decay = jnp.exp(jnp.where(causal, cum_b - cum_t[h:h + 1, :], -1e30))
            w = scores * decay * dt_t[h:h + 1, :]
            parts.append(jnp.dot(w.astype(BF16), u, preferred_element_type=F32))
            cums.append(cum_b)
            dts.append(jnp.broadcast_to(dt[:, h:h + 1], (T, 128)))
        cum_p = jnp.where(left, cums[0], cums[1])
        dt_p = jnp.where(left, dts[0], dts[1])
        end = cum_p[T - 1:T, :]
        y = jnp.where(left, parts[0], parts[1]) + jnp.exp(cum_p) * prev[:, lanes] + prm_ref[6:7, lanes] * u32
        xw = (u32 * (jnp.exp(end - cum_p) * dt_p)).astype(BF16)
        state[:, lanes] = jnp.exp(end) * state[:, lanes] + jnp.dot(b_t, xw, preferred_element_type=F32)
        gated = y * silu(z_ref[0, :, lanes].astype(F32))
        qs[:, lanes] = gated
        sq = sq + gated * gated

    inv = lax.rsqrt(jnp.sum(sq, axis=1, keepdims=True) / width + 1e-5)
    q_ref[...] = (qs[...] * inv * prm_ref[5:6, :]).astype(BF16)


def ssd_call(zx, bc, r, prm, bcp, hp):
    n_tok, inner = zx.shape[1], zx.shape[2]
    groups = bc.shape[0]
    width = inner // groups
    n_bc = bc.shape[2]
    T = CHUNK
    return pl.pallas_call(
        ssd_kernel,
        grid=(groups, n_tok // T),
        in_specs=[
            pl.BlockSpec((1, T, width), lambda g, c: (0, c, g)),
            pl.BlockSpec((1, T, width), lambda g, c: (1, c, g)),
            pl.BlockSpec((1, T, n_bc), lambda g, c: (g, c, 0)),
            pl.BlockSpec((1, T, 128), lambda g, c: (g, c, 0)),
            pl.BlockSpec((8, width), lambda g, c: (0, g)),
            pl.BlockSpec((1, 8, n_bc), lambda g, c: (g, 0, 0)),
            pl.BlockSpec((1, 8, 128), lambda g, c: (g, 0, 0)),
        ],
        out_specs=pl.BlockSpec((T, width), lambda g, c: (c, g)),
        out_shape=jax.ShapeDtypeStruct((n_tok, inner), BF16),
        scratch_shapes=[
            pltpu.VMEM((T + 8, width), F32),
            pltpu.VMEM((T + 8, n_bc), F32),
            pltpu.VMEM((n_bc // 2, width), F32),
            pltpu.VMEM((T, width), F32),
            pltpu.VMEM((T, width), F32),
        ],
        compiler_params=pltpu.CompilerParams(dimension_semantics=('arbitrary', 'arbitrary'), vmem_limit_bytes=48 * 2**20),
        cost_estimate=pl.CostEstimate(flops=8 * 10**9, bytes_accessed=14 * 2**20, transcendentals=10**7),
        name='ssd',
    )(zx, zx, bc, r, prm, bcp, hp)


def out_kernel(n_blk, rows, q_hbm, x_hbm, w_ref, out_ref, res_ref, qp, snd, own, rxs, rxx, ysnd, yrx, qsem, ss, rs, xs, xr, ys, yr):
    p, n = pl.program_id(0), pl.program_id(1)
    dp, sp, tp = lax.axis_index('dp'), lax.axis_index('sp'), lax.axis_index('tp')
    core = lax.rem(tp, 2)
    sib = tp + 1 - 2 * core
    across = lax.rem(tp + 2, 4)
    diag = lax.rem(sib + 2, 4)
    to_sib, to_x, to_y = (dp, sp, sib), (dp, sp, across), (dp, 1 - sp, tp)

    def q_copies(which):
        out = []
        for slot, quarter in enumerate(((diag, across), (sib, tp))[which]):
            for blk in range(2):
                src = q_hbm.at[pl.ds(pl.multiple_of(blk * 4 * rows + quarter * rows, rows), rows)]
                dst = qp.at[which, pl.ds((slot * 2 + blk) * rows, rows)]
                out.append(pltpu.make_async_copy(src, dst, qsem.at[which * 4 + slot * 2 + blk]))
        return out

    def res_copies():
        return [pltpu.make_async_copy(
            x_hbm.at[pl.ds(pl.multiple_of(blk * 4 * rows + tp * rows, rows), rows)],
            res_ref.at[pl.ds(blk * rows, rows)], qsem.at[8 + blk]) for blk in range(2)]

    def sib_copy(k, m):
        return pltpu.make_async_remote_copy(
            src_ref=snd.at[k, m], dst_ref=rxs.at[k, m], send_sem=ss.at[k, m], recv_sem=rs.at[k, m],
            device_id=to_sib, device_id_type=MESH)

    def x_copy(m):
        return pltpu.make_async_remote_copy(
            src_ref=own.at[0, m], dst_ref=rxx.at[m], send_sem=xs.at[m], recv_sem=xr.at[m],
            device_id=to_x, device_id_type=MESH)

    def y_copy(m):
        return pltpu.make_async_remote_copy(
            src_ref=ysnd.at[m], dst_ref=yrx.at[m], send_sem=ys.at[m], recv_sem=yr.at[m],
            device_id=to_y, device_id_type=MESH)

    @pl.when(jnp.logical_and(p == 0, n == 0))
    def _():
        for copy in q_copies(0) + q_copies(1) + res_copies():
            copy.start()
        barrier = pltpu.get_barrier_semaphore()
        for peer in (to_sib, to_x, to_y):
            pl.semaphore_signal(barrier, inc=1, device_id=peer, device_id_type=MESH)
        pl.semaphore_wait(barrier, 3)
        for copy in q_copies(0) + q_copies(1) + res_copies():
            copy.wait()

    acc = jnp.dot(qp[p], w_ref[...], preferred_element_type=F32)
    snd[p, n] = acc[:2 * rows]
    own[p, n] = acc[2 * rows:]
    sib_copy(p, n).start()

    def forward(m):
        sib_copy(0, m).wait_recv()
        own[0, m] = own[0, m] + rxs[0, m]
        x_copy(m).start()

    @pl.when(jnp.logical_and(p == 0, n >= 1))
    def _():
        forward(n - 1)

    @pl.when(jnp.logical_and(p == 1, n == 0))
    def _():
        forward(n_blk - 1)

    @pl.when(jnp.logical_and(p == 1, n == n_blk - 1))
    def _():
        def finish(m, carry):
            sib_copy(1, m).wait_recv()
            x_copy(m).wait_recv()
            cols = pl.ds(pl.multiple_of(m * NB, NB), NB)
            for half, blk in enumerate((sp, 1 - sp)):
                part = pl.ds(pl.multiple_of(blk * rows, rows), rows)
                total = own[1, m, part] + rxs[1, m, part] + rxx[m, part] + res_ref[part, cols].astype(F32)
                if half == 0:
                    out_ref[sp, :, cols] = total.astype(BF16)
                else:
                    ysnd[m] = total.astype(BF16)
            y_copy(m).start()
            return carry

        lax.fori_loop(0, n_blk, finish, 0)

        def drain(m, carry):
            y_copy(m).wait_recv()
            cols = pl.ds(pl.multiple_of(m * NB, NB), NB)
            out_ref[1 - sp, :, cols] = yrx[m]
            sib_copy(0, m).wait_send()
            sib_copy(1, m).wait_send()
            x_copy(m).wait_send()
            y_copy(m).wait_send()
            return carry

        lax.fori_loop(0, n_blk, drain, 0)


def out_call(q, x_all, w_out, rows):
    depth, d_model = w_out.shape
    n_blk = d_model // NB
    blk2 = (2, n_blk, 2 * rows, NB)
    return pl.pallas_call(
        functools.partial(out_kernel, n_blk, rows),
        grid=(2, n_blk),
        in_specs=[
            pl.BlockSpec(memory_space=pl.ANY),
            pl.BlockSpec(memory_space=pl.ANY),
            pl.BlockSpec((depth, NB), lambda p, n: (0, n)),
        ],
        out_specs=pl.BlockSpec(memory_space=pltpu.VMEM),
        out_shape=jax.ShapeDtypeStruct((2, rows, d_model), BF16),
        scratch_shapes=[
            pltpu.VMEM((2 * rows, d_model), BF16),
            pltpu.VMEM((2, 4 * rows, depth), BF16),
            pltpu.VMEM(blk2, F32),
            pltpu.VMEM(blk2, F32),
            pltpu.VMEM(blk2, F32),
            pltpu.VMEM(blk2[1:], F32),
            pltpu.VMEM((n_blk, rows, NB), BF16),
            pltpu.VMEM((n_blk, rows, NB), BF16),
            pltpu.SemaphoreType.DMA((10,)),
            pltpu.SemaphoreType.DMA((2, n_blk)),
            pltpu.SemaphoreType.DMA((2, n_blk)),
            pltpu.SemaphoreType.DMA((n_blk,)),
            pltpu.SemaphoreType.DMA((n_blk,)),
            pltpu.SemaphoreType.DMA((n_blk,)),
            pltpu.SemaphoreType.DMA((n_blk,)),
        ],
        compiler_params=pltpu.CompilerParams(
            dimension_semantics=('arbitrary', 'arbitrary'), collective_id=1, has_side_effects=True, vmem_limit_bytes=60 * 2**20),
        cost_estimate=pl.CostEstimate(flops=35 * 10**9, bytes_accessed=140 * 2**20, transcendentals=0),
        name='out_proj',
    )(q, x_all, w_out)


def gather_kernel(n_chunk, x_hbm, w_ref, wdt_ref, xall_ref, bc_ref, r_ref, xg, wv, acc, racc, lsem, wsem, osem, ss, rs):
    dp, sp, tp = lax.axis_index('dp'), lax.axis_index('sp'), lax.axis_index('tp')
    rows = x_hbm.shape[1]
    width = xg.shape[2]
    half = width // 2
    core = lax.rem(tp, 2)
    sib = tp + 1 - 2 * core
    across = lax.rem(tp + 2, 4)
    diag = lax.rem(sib + 2, 4)
    to_sib, to_x, to_y = (dp, sp, sib), (dp, sp, across), (dp, 1 - sp, tp)

    def slot(k, blk, owner):
        return xg.at[k, pl.ds(pl.multiple_of((blk * 4 + owner) * rows, rows), rows)]

    def columns(seq, k):
        return x_hbm.at[seq, :, pl.ds(k * width, width)]

    def local(k):
        return pltpu.make_async_copy(columns(sp, k), slot(k, sp, tp), lsem.at[k])

    def weights(k):
        return [pltpu.make_async_copy(
            w_ref.at[pl.ds(k * half, half), par, c, j, tp], wv.at[k, par, c, j], wsem.at[k, par * 4 + c * 2 + j])
            for par in range(2) for c in range(2) for j in range(2)]

    def send(kind, k):
        source, target = [
            (None, to_y),
            ((sp, tp), to_x), ((1 - sp, tp), to_x),
            ((sp, tp), to_sib), ((1 - sp, tp), to_sib),
            ((sp, across), to_sib), ((1 - sp, across), to_sib),
        ][kind]
        if source is None:
            src, dst = columns(1 - sp, k), slot(k, sp, tp)
        else:
            src = dst = slot(k, *source)
        return pltpu.make_async_remote_copy(
            src_ref=src, dst_ref=dst, send_sem=ss.at[kind, k], recv_sem=rs.at[kind, k],
            device_id=target, device_id_type=MESH)

    def arrived(kind, k):
        blk, owner = [(1 - sp, tp), (sp, across), (1 - sp, across), (sp, sib), (1 - sp, sib), (sp, diag), (1 - sp, diag)][kind]
        here = slot(k, blk, owner)
        pltpu.make_async_remote_copy(
            src_ref=here, dst_ref=here, send_sem=ss.at[kind, k], recv_sem=rs.at[kind, k],
            device_id=to_sib, device_id_type=MESH).wait_recv()

    def store(k):
        return pltpu.make_async_copy(xg.at[k], xall_ref.at[:, pl.ds(k * width, width)], osem.at[k])

    for k in range(n_chunk):
        local(k).start()
    for k in range(n_chunk):
        for copy in weights(k):
            copy.start()
    barrier = pltpu.get_barrier_semaphore()
    for peer in (to_sib, to_x, to_y):
        pl.semaphore_signal(barrier, inc=1, device_id=peer, device_id_type=MESH)
    pl.semaphore_wait(barrier, 3)

    def own_out(k):
        local(k).wait()
        send(1, k).start()
        send(3, k).start()

    def swapped_out(k):
        arrived(0, k)
        send(2, k).start()
        send(4, k).start()

    step = 512
    even = lax.rem(lax.broadcasted_iota(jnp.int32, (step // 8, 8, 128), 1), 2) == 0

    def compute(k):
        arrived(1, k)
        send(5, k).start()
        arrived(2, k)
        send(6, k).start()
        for copy in weights(k):
            copy.wait()
        for kind in range(3, 7):
            arrived(kind, k)
        store(k).start()

        def part(i, carry):
            span = pl.ds(pl.multiple_of(i * step, step), step)
            lhs = xg[k, :, span]
            for c in range(2):
                first, second = [], []
                for j in range(2):
                    a = wv.at[k, 0, c, j].reshape(width, 128)[span, :].astype(F32).reshape(step // 8, 8, 128)
                    b = wv.at[k, 1, c, j].reshape(width, 128)[span, :].astype(F32).reshape(step // 8, 8, 128)
                    first.append(jnp.where(even, a, pltpu.roll(b, 1, 1)).reshape(step, 128).astype(BF16))
                    second.append(jnp.where(even, pltpu.roll(a, 7, 1), b).reshape(step, 128).astype(BF16))
                for g, pieces in enumerate((first, second)):
                    acc[g, c] += jnp.dot(lhs, jnp.concatenate(pieces, axis=1), preferred_element_type=F32)
            return carry

        lax.fori_loop(0, width // step, part, 0)
        racc[...] += lax.dot_general(
            xg[k], wdt_ref[:, k * width:(k + 1) * width], (((1,), (1,)), ((), ())), preferred_element_type=F32)

    for k in range(n_chunk):
        send(0, k).start()
    acc[...] = jnp.zeros_like(acc)
    racc[...] = jnp.zeros_like(racc)
    own_out(0)
    own_out(1)
    swapped_out(0)
    own_out(2)
    swapped_out(1)
    own_out(3)
    compute(0)
    swapped_out(2)
    compute(1)
    swapped_out(3)
    compute(2)
    compute(3)

    for g in range(2):
        for c in range(2):
            bc_ref[g, :, c * 256:(c + 1) * 256] = acc[g, c].astype(BF16)
    r_ref[...] = racc[...].astype(BF16)
    for k in range(n_chunk):
        for kind in range(7):
            send(kind, k).wait_send()
        store(k).wait()


def gather_call(x_loc, w_bc, w_dt):
    n_seq, rows, d_model = x_loc.shape
    n_tok = 8 * rows
    n_chunk = 4
    width = d_model // n_chunk
    heads = w_dt.shape[1]
    w_view = w_bc.reshape(d_model // 2, 2, 2, 4, 2, 2, 128).transpose(0, 1, 2, 5, 3, 4, 6)
    anywhere = pl.BlockSpec(memory_space=pl.ANY)
    vmem = pl.BlockSpec(memory_space=pltpu.VMEM)
    dma = pltpu.SemaphoreType.DMA
    return pl.pallas_call(
        functools.partial(gather_kernel, n_chunk),
        in_specs=[anywhere, anywhere, vmem],
        out_specs=(anywhere, vmem, vmem),
        out_shape=(
            jax.ShapeDtypeStruct((n_tok, d_model), BF16),
            jax.ShapeDtypeStruct((2, n_tok, 512), BF16),
            jax.ShapeDtypeStruct((n_tok, heads), BF16),
        ),
        scratch_shapes=[
            pltpu.VMEM((n_chunk, n_tok, width), BF16),
            pltpu.VMEM((n_chunk, 2, 2, 2, width // 2, 2, 128), BF16),
            pltpu.VMEM((2, 2, n_tok, 256), F32),
            pltpu.VMEM((n_tok, heads), F32),
            dma((n_chunk,)), dma((n_chunk, 8)), dma((n_chunk,)), dma((7, n_chunk)), dma((7, n_chunk)),
        ],
        compiler_params=pltpu.CompilerParams(collective_id=2, has_side_effects=True, vmem_limit_bytes=48 * 2**20),
        cost_estimate=pl.CostEstimate(flops=10**10, bytes_accessed=30 * 2**20, transcendentals=0),
        name='gather_bc',
    )(x_loc, w_view, w_dt.T)


def solution(mesh):
    tp_size = mesh.shape['tp']
    tok_spec = P('dp', ('sp', 'tp'), None)

    def local_layer(x_loc, w_zx, w_dt, w_bc, conv_x, conv_bc, bias_x, bias_bc, a_log, dt_bias, d_skip, norm_w, w_out):
        rows, d_model = x_loc.shape[1], x_loc.shape[2]
        groups = w_bc.shape[2]
        heads = a_log.shape[0]
        inner = w_zx.shape[2]
        g_loc = groups // tp_size
        per_group = heads // g_loc
        sp, tp = lax.axis_index('sp'), lax.axis_index('tp')
        first = tp * g_loc
        conv_bc_loc = lax.dynamic_slice_in_dim(conv_bc, first, g_loc, axis=2)
        bias_bc_loc = lax.dynamic_slice_in_dim(bias_bc, first, g_loc, axis=1)

        x_all, bc, r = gather_call(x_loc, w_bc, w_dt)
        n_tok = x_all.shape[0]
        n_state = w_bc.shape[3]
        r = jnp.moveaxis(r.reshape(n_tok, g_loc, per_group), 1, 0)
        r = jnp.pad(r, ((0, 0), (0, 0), (0, 128 - per_group)))
        zx = jnp.einsum('md,dcn->cmn', x_all, w_zx, preferred_element_type=F32).astype(BF16)

        skip = jnp.repeat(d_skip, inner // heads)
        prm = jnp.concatenate([conv_x.astype(F32), bias_x.astype(F32)[None], norm_w.astype(F32)[None], skip[None], jnp.zeros((1, inner), F32)])
        taps = jnp.moveaxis(conv_bc_loc.astype(F32), 2, 0).reshape(g_loc, 4, 2 * n_state)
        bias = jnp.moveaxis(bias_bc_loc.astype(F32), 1, 0).reshape(g_loc, 1, 2 * n_state)
        bcp = jnp.concatenate([taps, bias, jnp.zeros((g_loc, 3, 2 * n_state), F32)], axis=1)
        hp = jnp.stack([dt_bias, -jnp.exp(a_log)]).reshape(2, g_loc, per_group)
        hp = jnp.pad(jnp.moveaxis(hp, 1, 0), ((0, 0), (0, 6), (0, 128 - per_group)))

        q = ssd_call(zx, bc, r, prm, bcp, hp)
        return out_call(q, x_all, w_out, rows)

    in_specs = (tok_spec, P(None, None, 'tp'), P(None, 'tp'), P(), P(None, 'tp'), P(), P('tp'), P(), P('tp'), P('tp'), P('tp'), P('tp'), P('tp', None))
    return jax.shard_map(local_layer, mesh=mesh, in_specs=in_specs, out_specs=tok_spec, check_vma=False)
```

```python
import functools

import jax
import jax.numpy as jnp
from jax import lax
from jax.experimental import pallas as pl
from jax.experimental.pallas import tpu as pltpu
from jax.sharding import PartitionSpec as P

MESH = pl.DeviceIdType.MESH
CHUNK = 128
NB = 512
F32 = jnp.float32
BF16 = jnp.bfloat16


def silu(v):
    return v * jax.nn.sigmoid(v)


def ssd_step(g, chunk, tp, z_ref, x_ref, bc_ref, r_ref, cx_ref, nb_ref, hp_ref, bcs, q_out, xs, bs, xtail, btail, state, qs, prev):
    T = CHUNK
    width = xs.shape[1]
    n_state = bs.shape[1] // 2

    @pl.when(chunk == 0)
    def _():
        xtail[g] = jnp.zeros_like(xtail[g])
        btail[g] = jnp.zeros_like(btail[g])
        state[g] = jnp.zeros_like(state[g])

    xs[0:8, :] = xtail[g]
    bs[0:8, :] = btail[g]
    xs[8:8 + T, :] = x_ref[0].astype(F32)
    bs[8:8 + T, :] = bc_ref[0].astype(F32)
    xtail[g] = xs[T:T + 8, :]
    btail[g] = bs[T:T + 8, :]

    halves = []
    group = pl.ds(tp * 2 + g, 1)
    for c in range(2):
        lanes = slice(c * n_state, (c + 1) * n_state)
        conv = bcs[4, c, group, :]
        for tap in range(4):
            conv = conv + bs[5 + tap:5 + tap + T, lanes] * bcs[tap, c, group, :]
        halves.append(silu(conv).astype(BF16))
    b_mat, c_mat = halves
    scores = lax.dot_general(c_mat, b_mat, (((1,), (1,)), ((), ())), preferred_element_type=F32)
    b_t = jnp.transpose(b_mat.astype(F32)).astype(BF16)

    dt = jax.nn.softplus(r_ref[0].astype(F32) + hp_ref[0, 0:1, :])
    log_a = -jnp.exp(hp_ref[0, 1:2, :]) * dt
    row = lax.broadcasted_iota(jnp.int32, (T, T), 0)
    col = lax.broadcasted_iota(jnp.int32, (T, T), 1)
    causal = row >= col
    cum = jnp.dot(causal.astype(F32), log_a, preferred_element_type=F32, precision=lax.Precision.HIGHEST)
    cum_t = jnp.transpose(cum)
    dt_t = jnp.transpose(dt)
    left = lax.broadcasted_iota(jnp.int32, (T, 128), 1) < 64
    prev[...] = jnp.dot(c_mat, state[g].astype(BF16), preferred_element_type=F32)
    sq = jnp.zeros((T, 128), F32)

    for pair in range(width // 128):
        lanes = slice(pair * 128, pair * 128 + 128)
        conv = nb_ref[0:1, lanes].astype(F32)
        for tap in range(4):
            conv = conv + xs[5 + tap:5 + tap + T, lanes] * cx_ref[tap:tap + 1, lanes].astype(F32)
        u = silu(conv).astype(BF16)
        u32 = u.astype(F32)
        parts, cums, dts, skips = [], [], [], []
        for half in range(2):
            h = 2 * pair + half
            cum_b = jnp.broadcast_to(cum[:, h:h + 1], (T, 128))
            decay = jnp.exp(jnp.where(causal, cum_b - cum_t[h:h + 1, :], -1e30))
            w = scores * decay * dt_t[h:h + 1, :]
            parts.append(jnp.dot(w.astype(BF16), u, preferred_element_type=F32))
            cums.append(cum_b)
            dts.append(jnp.broadcast_to(dt[:, h:h + 1], (T, 128)))
            skips.append(jnp.broadcast_to(hp_ref[0, 2:3, h:h + 1], (1, 128)))
        cum_p = jnp.where(left, cums[0], cums[1])
        dt_p = jnp.where(left, dts[0], dts[1])
        skip = jnp.where(left[0:1], skips[0], skips[1])
        end = cum_p[T - 1:T, :]
        y = jnp.where(left, parts[0], parts[1]) + jnp.exp(cum_p) * prev[:, lanes] + skip * u32
        xw = (u32 * (jnp.exp(end - cum_p) * dt_p)).astype(BF16)
        state[g, :, lanes] = jnp.exp(end) * state[g, :, lanes] + jnp.dot(b_t, xw, preferred_element_type=F32)
        gated = y * silu(z_ref[0, :, lanes].astype(F32))
        qs[:, lanes] = gated
        sq = sq + gated * gated

    inv = lax.rsqrt(jnp.sum(sq, axis=1, keepdims=True) / width + 1e-5)
    cols = pl.ds(pl.multiple_of(g * width, width), width)
    q_out[lax.rem(chunk, 2), chunk // 2, :, cols] = (qs[...] * inv * nb_ref[1:2, :].astype(F32)).astype(BF16)


def scan_index(s, n_blk):
    return jnp.where(s < 4, s, jnp.where(s < 4 + n_blk, 4, jnp.minimum(s - n_blk, 7)))


def column_index(s, n_blk):
    first = jnp.where(s < 4, 0, s - 4)
    second = jnp.where(s < 8 + n_blk, 0, s - 8 - n_blk)
    last = s - 8 - 2 * n_blk
    return jnp.where(s < 4 + n_blk, first, jnp.where(s < 8 + 2 * n_blk, second, last))


def out_kernel(n_blk, rows, x_hbm, cbc_ref, bbc_ref, z_ref, x_ref, bc_ref, r_ref, cx_ref, nb_ref, hp_ref, w_ref, out_ref,
               res_ref, bcs, qv, xs, bs, xtail, btail, state, qs, prev, a1, rs1, rxx, a2, rs2, ysnd, yrx,
               lsem, s1, r1, s2, r2, sx, rx, sy, ry):
    s = pl.program_id(0)
    dp, sp, tp = lax.axis_index('dp'), lax.axis_index('sp'), lax.axis_index('tp')
    core = lax.rem(tp, 2)
    chip = tp // 2
    to_sib, to_x, to_y = (dp, sp, tp + 1 - 2 * core), (dp, sp, lax.rem(tp + 2, 4)), (dp, 1 - sp, tp)

    def res_copies():
        return [pltpu.make_async_copy(
            x_hbm.at[pl.ds(pl.multiple_of(blk * 4 * rows + tp * rows, rows), rows)],
            res_ref.at[blk], lsem.at[blk]) for blk in range(2)]

    def remote(src, dst, send_sem, recv_sem, peer):
        return pltpu.make_async_remote_copy(
            src_ref=src, dst_ref=dst, send_sem=send_sem, recv_sem=recv_sem, device_id=peer, device_id_type=MESH)

    def sib_first(h, m):
        return remote(a1.at[h, m, 1 - core], rs1.at[h, m], s1.at[h, m], r1.at[h, m], to_sib)

    def sib_second(m):
        return remote(a2.at[m, 1 - core], rs2.at[m], s2.at[m], r2.at[m], to_sib)

    def x_copy(h, m):
        return remote(a1.at[h, m, core], rxx.at[h, m], sx.at[h, m], rx.at[h, m], to_x)

    def y_copy(m):
        return remote(ysnd.at[m], yrx.at[m], sy.at[m], ry.at[m], to_y)

    @pl.when(s == 0)
    def _():
        for copy in res_copies():
            copy.start()
        barrier = pltpu.get_barrier_semaphore()
        for peer in (to_sib, to_x, to_y):
            pl.semaphore_signal(barrier, inc=1, device_id=peer, device_id_type=MESH)
        pl.semaphore_wait(barrier, 3)
        for copy in res_copies():
            copy.wait()
        for tap in range(4):
            bcs[tap] = cbc_ref[tap].astype(F32)
        bcs[4] = bbc_ref[...].astype(F32)

    def forward(h, m):
        sib_first(h, m).wait_recv()
        a1[h, m, core] = a1[h, m, core] + rs1[h, m]
        x_copy(h, m).start()

    @pl.when(s == 4 + n_blk)
    def _():
        forward(0, n_blk - 1)

    @pl.when(s == 8 + 2 * n_blk)
    def _():
        forward(1, n_blk - 1)

    scanning = jnp.logical_or(s < 4, jnp.logical_and(s >= 4 + n_blk, s < 8 + n_blk))

    @pl.when(scanning)
    def _():
        i = scan_index(s, n_blk)
        g = lax.rem(i, 4) // 2
        chunk = (i // 4) * 2 + lax.rem(i, 2)
        ssd_step(g, chunk, tp, z_ref, x_ref, bc_ref, r_ref, cx_ref, nb_ref, hp_ref, bcs, qv, xs, bs, xtail, btail, state, qs, prev)

    @pl.when(jnp.logical_and(jnp.logical_not(scanning), s < 8 + 2 * n_blk))
    def _():
        n = column_index(s, n_blk)
        h = jnp.where(s < 4 + n_blk, 0, 1)
        acc = jnp.dot(qv[1 - chip, h], w_ref[...], preferred_element_type=F32)
        a1[h, n, 0] = acc[:rows]
        a1[h, n, 1] = acc[rows:]
        sib_first(h, n).start()

        @pl.when(n >= 1)
        def _():
            forward(h, n - 1)

    @pl.when(s >= 8 + 2 * n_blk)
    def _():
        n = column_index(s, n_blk)
        acc = jnp.dot(qv[chip].reshape(4 * rows, qv.shape[3]), w_ref[...], preferred_element_type=F32)
        for h in range(2):
            for c in range(2):
                a2[n, c, h] = acc[(2 * h + c) * rows:(2 * h + c + 1) * rows]
        sib_second(n).start()

    @pl.when(s == 7 + 3 * n_blk)
    def _():
        for h in range(2):
            def finish(m, carry):
                if h == 0:
                    sib_second(m).wait_recv()
                x_copy(h, m).wait_recv()
                cols = pl.ds(pl.multiple_of(m * NB, NB), NB)
                total = a2[m, core, h] + rs2[m, h] + rxx[h, m] + res_ref[h, :, cols].astype(F32)

                @pl.when(sp == h)
                def _():
                    out_ref[h, :, cols] = total.astype(BF16)

                @pl.when(sp != h)
                def _():
                    ysnd[m] = total.astype(BF16)
                    y_copy(m).start()

                return carry

            lax.fori_loop(0, n_blk, finish, 0)

        def drain(m, carry):
            y_copy(m).wait_recv()
            cols = pl.ds(pl.multiple_of(m * NB, NB), NB)
            out_ref[1 - sp, :, cols] = yrx[m]
            for h in range(2):
                sib_first(h, m).wait_send()
                x_copy(h, m).wait_send()
            sib_second(m).wait_send()
            y_copy(m).wait_send()
            return carry

        lax.fori_loop(0, n_blk, drain, 0)


def out_call(x_all, zx, bc, r, conv_x, conv_bc, bias_bc, nb, hp, w_out, rows):
    depth, d_model = w_out.shape
    n_blk = d_model // NB
    inner = zx.shape[2]
    groups = bc.shape[0]
    width = inner // groups
    n_bc = bc.shape[2]
    T = CHUNK
    dma = pltpu.SemaphoreType.DMA

    def at(make):
        def index(s):
            i = scan_index(s, n_blk)
            return make(lax.rem(i, 4) // 2, (i // 4) * 2 + lax.rem(i, 2))
        return index

    vmem = pl.BlockSpec(memory_space=pltpu.VMEM)
    return pl.pallas_call(
        functools.partial(out_kernel, n_blk, rows),
        grid=(8 + 3 * n_blk,),
        in_specs=[
            pl.BlockSpec(memory_space=pl.ANY),
            vmem,
            vmem,
            pl.BlockSpec((1, T, width), at(lambda g, c: (0, c, g))),
            pl.BlockSpec((1, T, width), at(lambda g, c: (1, c, g))),
            pl.BlockSpec((1, T, n_bc), at(lambda g, c: (g, c, 0))),
            pl.BlockSpec((1, T, 128), at(lambda g, c: (g, c, 0))),
            pl.BlockSpec((4, width), at(lambda g, c: (0, g))),
            pl.BlockSpec((2, width), at(lambda g, c: (0, g))),
            pl.BlockSpec((1, 3, 128), at(lambda g, c: (g, 0, 0))),
            pl.BlockSpec((depth, NB), lambda s: (0, column_index(s, n_blk))),
        ],
        out_specs=vmem,
        out_shape=jax.ShapeDtypeStruct((2, rows, d_model), BF16),
        scratch_shapes=[
            pltpu.VMEM((2, rows, d_model), BF16),
            pltpu.VMEM((5,) + conv_bc.shape[1:], F32),
            pltpu.VMEM((2, 2, T, inner), BF16),
            pltpu.VMEM((T + 8, width), F32),
            pltpu.VMEM((T + 8, n_bc), F32),
            pltpu.VMEM((groups, 8, width), F32),
            pltpu.VMEM((groups, 8, n_bc), F32),
            pltpu.VMEM((groups, n_bc // 2, width), F32),
            pltpu.VMEM((T, width), F32),
            pltpu.VMEM((T, width), F32),
            pltpu.VMEM((2, n_blk, 2, rows, NB), F32),
            pltpu.VMEM((2, n_blk, rows, NB), F32),
            pltpu.VMEM((2, n_blk, rows, NB), F32),
            pltpu.VMEM((n_blk, 2, 2, rows, NB), F32),
            pltpu.VMEM((n_blk, 2, rows, NB), F32),
            pltpu.VMEM((n_blk, rows, NB), BF16),
            pltpu.VMEM((n_blk, rows, NB), BF16),
            dma((2,)), dma((2, n_blk)), dma((2, n_blk)), dma((n_blk,)), dma((n_blk,)),
            dma((2, n_blk)), dma((2, n_blk)), dma((n_blk,)), dma((n_blk,)),
        ],
        compiler_params=pltpu.CompilerParams(
            dimension_semantics=('arbitrary',), collective_id=1, has_side_effects=True, vmem_limit_bytes=67043328),
        cost_estimate=pl.CostEstimate(flops=43 * 10**9, bytes_accessed=220 * 2**20, transcendentals=10**7),
        name='scan_out',
    )(x_all, conv_bc, bias_bc, zx, zx, bc, r, conv_x, nb, hp, w_out)


def gather_kernel(n_chunk, x_hbm, w_ref, wdt_ref, xall_ref, bc_ref, r_ref, xg, wv, acc, racc, lsem, wsem, osem, ss, rs):
    dp, sp, tp = lax.axis_index('dp'), lax.axis_index('sp'), lax.axis_index('tp')
    rows = x_hbm.shape[1]
    width = xg.shape[2]
    half = width // 2
    core = lax.rem(tp, 2)
    sib = tp + 1 - 2 * core
    across = lax.rem(tp + 2, 4)
    diag = lax.rem(sib + 2, 4)
    to_sib, to_x, to_y = (dp, sp, sib), (dp, sp, across), (dp, 1 - sp, tp)

    def slot(k, blk, owner):
        return xg.at[k, pl.ds(pl.multiple_of((blk * 4 + owner) * rows, rows), rows)]

    def columns(seq, k):
        return x_hbm.at[seq, :, pl.ds(k * width, width)]

    def local(k):
        return pltpu.make_async_copy(columns(sp, k), slot(k, sp, tp), lsem.at[k])

    def weights(k):
        return [pltpu.make_async_copy(
            w_ref.at[pl.ds(k * half, half), par, c, j, tp], wv.at[k, par, c, j], wsem.at[k, par * 4 + c * 2 + j])
            for par in range(2) for c in range(2) for j in range(2)]

    def send(kind, k):
        source, target = [
            (None, to_y),
            ((sp, tp), to_x), ((1 - sp, tp), to_x),
            ((sp, tp), to_sib), ((1 - sp, tp), to_sib),
            ((sp, across), to_sib), ((1 - sp, across), to_sib),
        ][kind]
        if source is None:
            src, dst = columns(1 - sp, k), slot(k, sp, tp)
        else:
            src = dst = slot(k, *source)
        return pltpu.make_async_remote_copy(
            src_ref=src, dst_ref=dst, send_sem=ss.at[kind, k], recv_sem=rs.at[kind, k],
            device_id=target, device_id_type=MESH)

    def arrived(kind, k):
        blk, owner = [(1 - sp, tp), (sp, across), (1 - sp, across), (sp, sib), (1 - sp, sib), (sp, diag), (1 - sp, diag)][kind]
        here = slot(k, blk, owner)
        pltpu.make_async_remote_copy(
            src_ref=here, dst_ref=here, send_sem=ss.at[kind, k], recv_sem=rs.at[kind, k],
            device_id=to_sib, device_id_type=MESH).wait_recv()

    def store(k):
        return pltpu.make_async_copy(xg.at[k], xall_ref.at[:, pl.ds(k * width, width)], osem.at[k])

    for k in range(n_chunk):
        local(k).start()
    for k in range(n_chunk):
        for copy in weights(k):
            copy.start()
    barrier = pltpu.get_barrier_semaphore()
    for peer in (to_sib, to_x, to_y):
        pl.semaphore_signal(barrier, inc=1, device_id=peer, device_id_type=MESH)
    pl.semaphore_wait(barrier, 3)

    def own_out(k):
        local(k).wait()
        send(1, k).start()
        send(3, k).start()

    def swapped_out(k):
        arrived(0, k)
        send(2, k).start()
        send(4, k).start()

    step = 512
    even = lax.rem(lax.broadcasted_iota(jnp.int32, (step // 8, 8, 128), 1), 2) == 0

    def compute(k):
        arrived(1, k)
        send(5, k).start()
        arrived(2, k)
        send(6, k).start()
        for copy in weights(k):
            copy.wait()
        for kind in range(3, 7):
            arrived(kind, k)
        store(k).start()

        def part(i, carry):
            span = pl.ds(pl.multiple_of(i * step, step), step)
            lhs = xg[k, :, span]
            for c in range(2):
                first, second = [], []
                for j in range(2):
                    a = wv.at[k, 0, c, j].reshape(width, 128)[span, :].astype(F32).reshape(step // 8, 8, 128)
                    b = wv.at[k, 1, c, j].reshape(width, 128)[span, :].astype(F32).reshape(step // 8, 8, 128)
                    first.append(jnp.where(even, a, pltpu.roll(b, 1, 1)).reshape(step, 128).astype(BF16))
                    second.append(jnp.where(even, pltpu.roll(a, 7, 1), b).reshape(step, 128).astype(BF16))
                for g, pieces in enumerate((first, second)):
                    acc[g, c] += jnp.dot(lhs, jnp.concatenate(pieces, axis=1), preferred_element_type=F32)
            return carry

        lax.fori_loop(0, width // step, part, 0)
        racc[...] += lax.dot_general(
            xg[k], wdt_ref[:, k * width:(k + 1) * width], (((1,), (1,)), ((), ())), preferred_element_type=F32)

    for k in range(n_chunk):
        send(0, k).start()
    acc[...] = jnp.zeros_like(acc)
    racc[...] = jnp.zeros_like(racc)
    own_out(0)
    own_out(1)
    swapped_out(0)
    own_out(2)
    swapped_out(1)
    own_out(3)
    compute(0)
    swapped_out(2)
    compute(1)
    swapped_out(3)
    compute(2)
    compute(3)

    for g in range(2):
        for c in range(2):
            bc_ref[g, :, c * 256:(c + 1) * 256] = acc[g, c].astype(BF16)
    per_group = racc.shape[1] // 2
    r_ref[...] = jnp.zeros_like(r_ref)
    for g in range(2):
        r_ref[g, :, 0:per_group] = racc[:, g * per_group:(g + 1) * per_group].astype(BF16)
    for k in range(n_chunk):
        for kind in range(7):
            send(kind, k).wait_send()
        store(k).wait()


def gather_call(x_loc, w_bc, w_dt):
    n_seq, rows, d_model = x_loc.shape
    n_tok = 8 * rows
    n_chunk = 4
    width = d_model // n_chunk
    heads = w_dt.shape[1]
    w_view = w_bc.reshape(d_model // 2, 2, 2, 4, 2, 2, 128).transpose(0, 1, 2, 5, 3, 4, 6)
    anywhere = pl.BlockSpec(memory_space=pl.ANY)
    vmem = pl.BlockSpec(memory_space=pltpu.VMEM)
    dma = pltpu.SemaphoreType.DMA
    return pl.pallas_call(
        functools.partial(gather_kernel, n_chunk),
        in_specs=[anywhere, anywhere, vmem],
        out_specs=(anywhere, vmem, vmem),
        out_shape=(
            jax.ShapeDtypeStruct((n_tok, d_model), BF16),
            jax.ShapeDtypeStruct((2, n_tok, 512), BF16),
            jax.ShapeDtypeStruct((2, n_tok, 128), BF16),
        ),
        scratch_shapes=[
            pltpu.VMEM((n_chunk, n_tok, width), BF16),
            pltpu.VMEM((n_chunk, 2, 2, 2, width // 2, 2, 128), BF16),
            pltpu.VMEM((2, 2, n_tok, 256), F32),
            pltpu.VMEM((n_tok, heads), F32),
            dma((n_chunk,)), dma((n_chunk, 8)), dma((n_chunk,)), dma((7, n_chunk)), dma((7, n_chunk)),
        ],
        compiler_params=pltpu.CompilerParams(collective_id=2, has_side_effects=True, vmem_limit_bytes=48 * 2**20),
        cost_estimate=pl.CostEstimate(flops=10**10, bytes_accessed=30 * 2**20, transcendentals=0),
        name='gather_bc',
    )(x_loc, w_view, w_dt.T)


def solution(mesh):
    tp_size = mesh.shape['tp']
    tok_spec = P('dp', ('sp', 'tp'), None)

    def local_layer(x_loc, w_zx, w_dt, w_bc, conv_x, conv_bc, bias_x, bias_bc, a_log, dt_bias, d_skip, norm_w, w_out):
        rows = x_loc.shape[1]
        g_loc = w_bc.shape[2] // tp_size
        x_all, bc, r = gather_call(x_loc, w_bc, w_dt)
        zx = jnp.einsum('md,dcn->cmn', x_all, w_zx, preferred_element_type=F32).astype(BF16)
        hp = jnp.stack([dt_bias.reshape(g_loc, -1), a_log.reshape(g_loc, -1), d_skip.reshape(g_loc, -1)], axis=1)
        hp = jnp.pad(hp, ((0, 0), (0, 0), (0, 128 - hp.shape[2])))
        nb = jnp.stack([bias_x, norm_w])
        return out_call(x_all, zx, bc, r, conv_x, conv_bc, bias_bc, nb, hp, w_out, rows)

    in_specs = (tok_spec, P(None, None, 'tp'), P(None, 'tp'), P(), P(None, 'tp'), P(), P('tp'), P(), P('tp'), P('tp'), P('tp'), P('tp'), P('tp', None))
    return jax.shard_map(local_layer, mesh=mesh, in_specs=in_specs, out_specs=tok_spec, check_vma=False)
```

```python
import functools

import jax
import jax.numpy as jnp
from jax import lax
from jax.experimental import pallas as pl
from jax.experimental.pallas import tpu as pltpu
from jax.sharding import PartitionSpec as P

MESH = pl.DeviceIdType.MESH
CHUNK = 128
NB = 512
F32 = jnp.float32
BF16 = jnp.bfloat16


def silu(v):
    return v * jax.nn.sigmoid(v)


def ssd_step(g, chunk, tp, z_ref, x_ref, bc_ref, r_ref, cx_ref, nb_ref, hp_ref, bcs, q_out, xs, bs, xtail, btail, state, qs, prev):
    T = CHUNK
    width = xs.shape[1]
    n_state = bs.shape[1] // 2

    @pl.when(chunk == 0)
    def _():
        xtail[g] = jnp.zeros_like(xtail[g])
        btail[g] = jnp.zeros_like(btail[g])
        state[g] = jnp.zeros_like(state[g])

    xs[0:8, :] = xtail[g]
    bs[0:8, :] = btail[g]
    xs[8:8 + T, :] = x_ref[0].astype(F32)
    bs[8:8 + T, :] = bc_ref[0].astype(F32)
    xtail[g] = xs[T:T + 8, :]
    btail[g] = bs[T:T + 8, :]

    halves = []
    group = pl.ds(tp * 2 + g, 1)
    for c in range(2):
        lanes = slice(c * n_state, (c + 1) * n_state)
        conv = bcs[4, c, group, :]
        for tap in range(4):
            conv = conv + bs[5 + tap:5 + tap + T, lanes] * bcs[tap, c, group, :]
        halves.append(silu(conv).astype(BF16))
    b_mat, c_mat = halves
    scores = lax.dot_general(c_mat, b_mat, (((1,), (1,)), ((), ())), preferred_element_type=F32)
    b_t = jnp.transpose(b_mat.astype(F32)).astype(BF16)

    dt = jax.nn.softplus(r_ref[0].astype(F32) + hp_ref[0, 0:1, :])
    log_a = -jnp.exp(hp_ref[0, 1:2, :]) * dt
    row = lax.broadcasted_iota(jnp.int32, (T, T), 0)
    col = lax.broadcasted_iota(jnp.int32, (T, T), 1)
    causal = row >= col
    cum = jnp.dot(causal.astype(F32), log_a, preferred_element_type=F32, precision=lax.Precision.HIGHEST)
    cum_t = jnp.transpose(cum)
    dt_t = jnp.transpose(dt)
    left = lax.broadcasted_iota(jnp.int32, (T, 128), 1) < 64
    prev[...] = jnp.dot(c_mat, state[g].astype(BF16), preferred_element_type=F32)
    sq = jnp.zeros((T, 128), F32)

    for pair in range(width // 128):
        lanes = slice(pair * 128, pair * 128 + 128)
        conv = nb_ref[0:1, lanes].astype(F32)
        for tap in range(4):
            conv = conv + xs[5 + tap:5 + tap + T, lanes] * cx_ref[tap:tap + 1, lanes].astype(F32)
        u = silu(conv).astype(BF16)
        u32 = u.astype(F32)
        parts, cums, dts, skips = [], [], [], []
        for half in range(2):
            h = 2 * pair + half
            cum_b = jnp.broadcast_to(cum[:, h:h + 1], (T, 128))
            decay = jnp.exp(jnp.where(causal, cum_b - cum_t[h:h + 1, :], -1e30))
            w = scores * decay * dt_t[h:h + 1, :]
            parts.append(jnp.dot(w.astype(BF16), u, preferred_element_type=F32))
            cums.append(cum_b)
            dts.append(jnp.broadcast_to(dt[:, h:h + 1], (T, 128)))
            skips.append(jnp.broadcast_to(hp_ref[0, 2:3, h:h + 1], (1, 128)))
        cum_p = jnp.where(left, cums[0], cums[1])
        dt_p = jnp.where(left, dts[0], dts[1])
        skip = jnp.where(left[0:1], skips[0], skips[1])
        end = cum_p[T - 1:T, :]
        y = jnp.where(left, parts[0], parts[1]) + jnp.exp(cum_p) * prev[:, lanes] + skip * u32
        xw = (u32 * (jnp.exp(end - cum_p) * dt_p)).astype(BF16)
        state[g, :, lanes] = jnp.exp(end) * state[g, :, lanes] + jnp.dot(b_t, xw, preferred_element_type=F32)
        gated = y * silu(z_ref[0, :, lanes].astype(F32))
        qs[:, lanes] = gated
        sq = sq + gated * gated

    inv = lax.rsqrt(jnp.sum(sq, axis=1, keepdims=True) / width + 1e-5)
    cols = pl.ds(pl.multiple_of(g * width, width), width)
    q_out[chunk // 2, lax.rem(chunk, 2), :, cols] = (qs[...] * inv * nb_ref[1:2, :].astype(F32)).astype(BF16)


def scan_index(s, n_blk):
    return jnp.where(s < 4, s, jnp.where(s < 4 + n_blk, 4, jnp.minimum(s - n_blk, 7)))


def column_index(s, n_blk):
    return jnp.where(s < 4 + n_blk, jnp.maximum(s - 4, 0), jnp.maximum(s - 8 - n_blk, 0))


def out_kernel(n_blk, rows, x_hbm, cbc_ref, bbc_ref, z_ref, x_ref, bc_ref, r_ref, cx_ref, nb_ref, hp_ref, w_ref, out_ref,
               res_ref, bcs, qv, xs, bs, xtail, btail, state, qs, prev, ab, rs1, rxx, rs2, ysnd, yrx,
               lsem, s1, r1, s2, r2, sx, rx, sy, ry):
    s = pl.program_id(0)
    dp, sp, tp = lax.axis_index('dp'), lax.axis_index('sp'), lax.axis_index('tp')
    core = lax.rem(tp, 2)
    chip = tp // 2
    to_sib, to_x, to_y = (dp, sp, tp + 1 - 2 * core), (dp, sp, lax.rem(tp + 2, 4)), (dp, 1 - sp, tp)

    def res_copies():
        return [pltpu.make_async_copy(
            x_hbm.at[pl.ds(pl.multiple_of(blk * 4 * rows + tp * rows, rows), rows)],
            res_ref.at[blk], lsem.at[blk]) for blk in range(2)]

    def remote(src, dst, send_sem, recv_sem, peer):
        return pltpu.make_async_remote_copy(
            src_ref=src, dst_ref=dst, send_sem=send_sem, recv_sem=recv_sem, device_id=peer, device_id_type=MESH)

    def sib_first(h, m):
        return remote(ab.at[h, m, 1 - chip, 1 - core], rs1.at[h, m], s1.at[h, m], r1.at[h, m], to_sib)

    def sib_second(h, m):
        return remote(ab.at[h, m, chip, 1 - core], rs2.at[h, m], s2.at[h, m], r2.at[h, m], to_sib)

    def x_copy(h, m):
        return remote(ab.at[h, m, 1 - chip, core], rxx.at[h, m], sx.at[h, m], rx.at[h, m], to_x)

    def y_copy(m):
        return remote(ysnd.at[m], yrx.at[m], sy.at[m], ry.at[m], to_y)

    @pl.when(s == 0)
    def _():
        for copy in res_copies():
            copy.start()
        barrier = pltpu.get_barrier_semaphore()
        for peer in (to_sib, to_x, to_y):
            pl.semaphore_signal(barrier, inc=1, device_id=peer, device_id_type=MESH)
        pl.semaphore_wait(barrier, 3)
        for copy in res_copies():
            copy.wait()
        for tap in range(4):
            bcs[tap] = cbc_ref[tap].astype(F32)
        bcs[4] = bbc_ref[...].astype(F32)

    def forward(h, m):
        sib_first(h, m).wait_recv()
        ab[h, m, 1 - chip, core] = ab[h, m, 1 - chip, core] + rs1[h, m]
        x_copy(h, m).start()

    @pl.when(s == 4 + n_blk)
    def _():
        forward(0, n_blk - 1)

    scanning = jnp.logical_or(s < 4, jnp.logical_and(s >= 4 + n_blk, s < 8 + n_blk))

    @pl.when(scanning)
    def _():
        i = scan_index(s, n_blk)
        g = lax.rem(i, 4) // 2
        chunk = (i // 4) * 2 + lax.rem(i, 2)
        ssd_step(g, chunk, tp, z_ref, x_ref, bc_ref, r_ref, cx_ref, nb_ref, hp_ref, bcs, qv, xs, bs, xtail, btail, state, qs, prev)

    @pl.when(jnp.logical_not(scanning))
    def _():
        n = column_index(s, n_blk)
        h = jnp.where(s < 4 + n_blk, 0, 1)
        acc = jnp.dot(qv[h].reshape(4 * rows, qv.shape[3]), w_ref[...], preferred_element_type=F32)
        for i in range(4):
            ab[h, n, i // 2, i % 2] = acc[i * rows:(i + 1) * rows]
        sib_first(h, n).start()
        sib_second(h, n).start()

        @pl.when(n >= 1)
        def _():
            forward(h, n - 1)

    @pl.when(s == 7 + 2 * n_blk)
    def _():
        forward(1, n_blk - 1)
        for h in range(2):
            def finish(m, carry):
                sib_second(h, m).wait_recv()
                x_copy(h, m).wait_recv()
                cols = pl.ds(pl.multiple_of(m * NB, NB), NB)
                total = ab[h, m, chip, core] + rs2[h, m] + rxx[h, m] + res_ref[h, :, cols].astype(F32)

                @pl.when(sp == h)
                def _():
                    out_ref[h, :, cols] = total.astype(BF16)

                @pl.when(sp != h)
                def _():
                    ysnd[m] = total.astype(BF16)
                    y_copy(m).start()

                return carry

            lax.fori_loop(0, n_blk, finish, 0)

        def drain(m, carry):
            y_copy(m).wait_recv()
            cols = pl.ds(pl.multiple_of(m * NB, NB), NB)
            out_ref[1 - sp, :, cols] = yrx[m]
            for h in range(2):
                sib_first(h, m).wait_send()
                x_copy(h, m).wait_send()
                sib_second(h, m).wait_send()
            y_copy(m).wait_send()
            return carry

        lax.fori_loop(0, n_blk, drain, 0)


def out_call(x_all, zx, bc, r, conv_x, conv_bc, bias_bc, nb, hp, w_out, rows):
    depth, d_model = w_out.shape
    n_blk = d_model // NB
    inner = zx.shape[2]
    groups = bc.shape[0]
    width = inner // groups
    n_bc = bc.shape[2]
    T = CHUNK
    dma = pltpu.SemaphoreType.DMA

    def at(make):
        def index(s):
            i = scan_index(s, n_blk)
            return make(lax.rem(i, 4) // 2, (i // 4) * 2 + lax.rem(i, 2))
        return index

    vmem = pl.BlockSpec(memory_space=pltpu.VMEM)
    return pl.pallas_call(
        functools.partial(out_kernel, n_blk, rows),
        grid=(8 + 2 * n_blk,),
        in_specs=[
            pl.BlockSpec(memory_space=pl.ANY),
            vmem,
            vmem,
            pl.BlockSpec((1, T, width), at(lambda g, c: (0, c, g))),
            pl.BlockSpec((1, T, width), at(lambda g, c: (1, c, g))),
            pl.BlockSpec((1, T, n_bc), at(lambda g, c: (g, c, 0))),
            pl.BlockSpec((1, T, 128), at(lambda g, c: (g, c, 0))),
            pl.BlockSpec((4, width), at(lambda g, c: (0, g))),
            pl.BlockSpec((2, width), at(lambda g, c: (0, g))),
            pl.BlockSpec((1, 3, 128), at(lambda g, c: (g, 0, 0))),
            pl.BlockSpec((depth, NB), lambda s: (0, column_index(s, n_blk))),
        ],
        out_specs=vmem,
        out_shape=jax.ShapeDtypeStruct((2, rows, d_model), BF16),
        scratch_shapes=[
            pltpu.VMEM((2, rows, d_model), BF16),
            pltpu.VMEM((5,) + conv_bc.shape[1:], F32),
            pltpu.VMEM((2, 2, T, inner), BF16),
            pltpu.VMEM((T + 8, width), F32),
            pltpu.VMEM((T + 8, n_bc), F32),
            pltpu.VMEM((groups, 8, width), F32),
            pltpu.VMEM((groups, 8, n_bc), F32),
            pltpu.VMEM((groups, n_bc // 2, width), F32),
            pltpu.VMEM((T, width), F32),
            pltpu.VMEM((T, width), F32),
            pltpu.VMEM((2, n_blk, 2, 2, rows, NB), F32),
            pltpu.VMEM((2, n_blk, rows, NB), F32),
            pltpu.VMEM((2, n_blk, rows, NB), F32),
            pltpu.VMEM((2, n_blk, rows, NB), F32),
            pltpu.VMEM((n_blk, rows, NB), BF16),
            pltpu.VMEM((n_blk, rows, NB), BF16),
            dma((2,)), dma((2, n_blk)), dma((2, n_blk)), dma((2, n_blk)), dma((2, n_blk)),
            dma((2, n_blk)), dma((2, n_blk)), dma((n_blk,)), dma((n_blk,)),
        ],
        compiler_params=pltpu.CompilerParams(
            dimension_semantics=('arbitrary',), collective_id=1, has_side_effects=True, vmem_limit_bytes=67043328),
        cost_estimate=pl.CostEstimate(flops=43 * 10**9, bytes_accessed=220 * 2**20, transcendentals=10**7),
        name='scan_out',
    )(x_all, conv_bc, bias_bc, zx, zx, bc, r, conv_x, nb, hp, w_out)


def gather_kernel(n_chunk, x_hbm, w_ref, wdt_ref, xall_ref, bc_ref, r_ref, xg, wv, acc, racc, lsem, wsem, osem, ss, rs):
    dp, sp, tp = lax.axis_index('dp'), lax.axis_index('sp'), lax.axis_index('tp')
    rows = x_hbm.shape[1]
    width = xg.shape[2]
    half = width // 2
    core = lax.rem(tp, 2)
    sib = tp + 1 - 2 * core
    across = lax.rem(tp + 2, 4)
    diag = lax.rem(sib + 2, 4)
    to_sib, to_x, to_y = (dp, sp, sib), (dp, sp, across), (dp, 1 - sp, tp)

    def slot(k, blk, owner):
        return xg.at[k, pl.ds(pl.multiple_of((blk * 4 + owner) * rows, rows), rows)]

    def columns(seq, k):
        return x_hbm.at[seq, :, pl.ds(k * width, width)]

    def local(k):
        return pltpu.make_async_copy(columns(sp, k), slot(k, sp, tp), lsem.at[k])

    def weights(k):
        return [pltpu.make_async_copy(
            w_ref.at[pl.ds(k * half, half), par, c, j, tp], wv.at[k, par, c, j], wsem.at[k, par * 4 + c * 2 + j])
            for par in range(2) for c in range(2) for j in range(2)]

    def send(kind, k):
        source, target = [
            (None, to_y),
            ((sp, tp), to_x), ((1 - sp, tp), to_x),
            ((sp, tp), to_sib), ((1 - sp, tp), to_sib),
            ((sp, across), to_sib), ((1 - sp, across), to_sib),
        ][kind]
        if source is None:
            src, dst = columns(1 - sp, k), slot(k, sp, tp)
        else:
            src = dst = slot(k, *source)
        return pltpu.make_async_remote_copy(
            src_ref=src, dst_ref=dst, send_sem=ss.at[kind, k], recv_sem=rs.at[kind, k],
            device_id=target, device_id_type=MESH)

    def arrived(kind, k):
        blk, owner = [(1 - sp, tp), (sp, across), (1 - sp, across), (sp, sib), (1 - sp, sib), (sp, diag), (1 - sp, diag)][kind]
        here = slot(k, blk, owner)
        pltpu.make_async_remote_copy(
            src_ref=here, dst_ref=here, send_sem=ss.at[kind, k], recv_sem=rs.at[kind, k],
            device_id=to_sib, device_id_type=MESH).wait_recv()

    def store(k):
        return pltpu.make_async_copy(xg.at[k], xall_ref.at[:, pl.ds(k * width, width)], osem.at[k])

    for k in range(n_chunk):
        local(k).start()
    for k in range(n_chunk):
        for copy in weights(k):
            copy.start()
    barrier = pltpu.get_barrier_semaphore()
    for peer in (to_sib, to_x, to_y):
        pl.semaphore_signal(barrier, inc=1, device_id=peer, device_id_type=MESH)
    pl.semaphore_wait(barrier, 3)

    def own_out(k):
        local(k).wait()
        send(1, k).start()
        send(3, k).start()

    def swapped_out(k):
        arrived(0, k)
        send(2, k).start()
        send(4, k).start()

    step = 512
    even = lax.rem(lax.broadcasted_iota(jnp.int32, (step // 8, 8, 128), 1), 2) == 0

    def compute(k):
        arrived(1, k)
        send(5, k).start()
        arrived(2, k)
        send(6, k).start()
        for copy in weights(k):
            copy.wait()
        for kind in range(3, 7):
            arrived(kind, k)
        store(k).start()

        def part(i, carry):
            span = pl.ds(pl.multiple_of(i * step, step), step)
            lhs = xg[k, :, span]
            for c in range(2):
                first, second = [], []
                for j in range(2):
                    a = wv.at[k, 0, c, j].reshape(width, 128)[span, :].astype(F32).reshape(step // 8, 8, 128)
                    b = wv.at[k, 1, c, j].reshape(width, 128)[span, :].astype(F32).reshape(step // 8, 8, 128)
                    first.append(jnp.where(even, a, pltpu.roll(b, 1, 1)).reshape(step, 128).astype(BF16))
                    second.append(jnp.where(even, pltpu.roll(a, 7, 1), b).reshape(step, 128).astype(BF16))
                for g, pieces in enumerate((first, second)):
                    acc[g, c] += jnp.dot(lhs, jnp.concatenate(pieces, axis=1), preferred_element_type=F32)
            return carry

        lax.fori_loop(0, width // step, part, 0)
        racc[...] += lax.dot_general(
            xg[k], wdt_ref[:, k * width:(k + 1) * width], (((1,), (1,)), ((), ())), preferred_element_type=F32)

    for k in range(n_chunk):
        send(0, k).start()
    acc[...] = jnp.zeros_like(acc)
    racc[...] = jnp.zeros_like(racc)
    own_out(0)
    own_out(1)
    swapped_out(0)
    own_out(2)
    swapped_out(1)
    own_out(3)
    compute(0)
    swapped_out(2)
    compute(1)
    swapped_out(3)
    compute(2)
    compute(3)

    for g in range(2):
        for c in range(2):
            bc_ref[g, :, c * 256:(c + 1) * 256] = acc[g, c].astype(BF16)
    per_group = racc.shape[1] // 2
    r_ref[...] = jnp.zeros_like(r_ref)
    for g in range(2):
        r_ref[g, :, 0:per_group] = racc[:, g * per_group:(g + 1) * per_group].astype(BF16)
    for k in range(n_chunk):
        for kind in range(7):
            send(kind, k).wait_send()
        store(k).wait()


def gather_call(x_loc, w_bc, w_dt):
    n_seq, rows, d_model = x_loc.shape
    n_tok = 8 * rows
    n_chunk = 4
    width = d_model // n_chunk
    heads = w_dt.shape[1]
    w_view = w_bc.reshape(d_model // 2, 2, 2, 4, 2, 2, 128).transpose(0, 1, 2, 5, 3, 4, 6)
    anywhere = pl.BlockSpec(memory_space=pl.ANY)
    vmem = pl.BlockSpec(memory_space=pltpu.VMEM)
    dma = pltpu.SemaphoreType.DMA
    return pl.pallas_call(
        functools.partial(gather_kernel, n_chunk),
        in_specs=[anywhere, anywhere, vmem],
        out_specs=(anywhere, vmem, vmem),
        out_shape=(
            jax.ShapeDtypeStruct((n_tok, d_model), BF16),
            jax.ShapeDtypeStruct((2, n_tok, 512), BF16),
            jax.ShapeDtypeStruct((2, n_tok, 128), BF16),
        ),
        scratch_shapes=[
            pltpu.VMEM((n_chunk, n_tok, width), BF16),
            pltpu.VMEM((n_chunk, 2, 2, 2, width // 2, 2, 128), BF16),
            pltpu.VMEM((2, 2, n_tok, 256), F32),
            pltpu.VMEM((n_tok, heads), F32),
            dma((n_chunk,)), dma((n_chunk, 8)), dma((n_chunk,)), dma((7, n_chunk)), dma((7, n_chunk)),
        ],
        compiler_params=pltpu.CompilerParams(collective_id=2, has_side_effects=True, vmem_limit_bytes=48 * 2**20),
        cost_estimate=pl.CostEstimate(flops=10**10, bytes_accessed=30 * 2**20, transcendentals=0),
        name='gather_bc',
    )(x_loc, w_view, w_dt.T)


def solution(mesh):
    tp_size = mesh.shape['tp']
    tok_spec = P('dp', ('sp', 'tp'), None)

    def local_layer(x_loc, w_zx, w_dt, w_bc, conv_x, conv_bc, bias_x, bias_bc, a_log, dt_bias, d_skip, norm_w, w_out):
        rows = x_loc.shape[1]
        g_loc = w_bc.shape[2] // tp_size
        x_all, bc, r = gather_call(x_loc, w_bc, w_dt)
        zx = jnp.einsum('md,dcn->cmn', x_all, w_zx, preferred_element_type=F32).astype(BF16)
        hp = jnp.stack([dt_bias.reshape(g_loc, -1), a_log.reshape(g_loc, -1), d_skip.reshape(g_loc, -1)], axis=1)
        hp = jnp.pad(hp, ((0, 0), (0, 0), (0, 128 - hp.shape[2])))
        nb = jnp.stack([bias_x, norm_w])
        return out_call(x_all, zx, bc, r, conv_x, conv_bc, bias_bc, nb, hp, w_out, rows)

    in_specs = (tok_spec, P(None, None, 'tp'), P(None, 'tp'), P(), P(None, 'tp'), P(), P('tp'), P(), P('tp'), P('tp'), P('tp'), P('tp'), P('tp', None))
    return jax.shard_map(local_layer, mesh=mesh, in_specs=in_specs, out_specs=tok_spec, check_vma=False)
```
